128 devices in a mesh: circ: 32 (over x_hi, y, z), side: 4 (over x_lo, core).
Axes of the slice: x: 4 (x_hi: 2, x_lo: 2; x = x_hi * 2 + x_lo), y: 4, z: 4, core: 2. Of those that a mesh axis runs over, the one named last changes fastest.
Arguments:
- field: float32 [4, 7, 7, 7, 8, 4096], P('side', None, None, None, None, 'circ'), may hold values from -6 to 6
- coeffs: float32 [4, 3, 7, 7, 7, 8, 4096], P('side', None, None, None, None, None, 'circ'), may hold values from 0.25 to 1.5
- reaction: float32 [4, 7, 7, 7, 8, 4096], P('side', None, None, None, None, 'circ'), may hold values from 0.25 to 8
- step_scale: float32 [4, 7, 7, 7, 8, 4096], P('side', None, None, None, None, 'circ'), may hold values from 0.0001 to 0.0003
- rotation: int32 [4], replicated, may hold values from 0 to 12287
Outputs:
- advanced: float32 [4, 7, 7, 7, 8, 4096], P('side', None, None, None, None, 'circ')
The draws below stay inside these ranges and needn't reach their ends.
Inputs may be any that keep to these rules, and one draw needn't show every extreme that they name: `rotation`: rotor position in units of one 3-th of an element's circumferential width.
All inputs are finite; a program needn't handle non-finite values.
Results may differ from the reference program's by a relative error of at most 0.0001.
Values sent between devices are 32-bit elements; how exact they have to be, the bound alone decides.
No kernel may reach another device: no remote copies, remote signals or barrier semaphores. Data moves between devices by JAX's collectives and lax.ppermute only.
A program may use at most 128 MiB of HBM per device.

```python
import math
import jax
import jax.numpy as jnp
import numpy as np
from jax import lax

NODES = 7
ER = 8
SUBSTEPS = 3
STEPS = 4
LAYERS = 4
NC = 4096


def plant(drawn, rng, smallest, top_value):
    dims = drawn.shape
    place = [jax.random.randint(jax.random.fold_in(rng, axis), (), 0, dims[axis]) for axis in range(len(dims))]
    drawn = drawn.at[tuple(place)].set(smallest)
    longest = dims.index(max(dims))
    place[longest] = (place[longest] + 1) % dims[longest]
    return drawn.at[tuple(place)].set(top_value)


def level_of(own_key, dims, shards, least, top_value):
    level, own = 1.0, jax.random.fold_in(own_key, 6)
    for axis_at, shards_of in shards:
        steps = jnp.exp(jax.random.uniform(jax.random.fold_in(own, axis_at), (shards_of,), jnp.float32, least / len(shards), top_value / len(shards)))
        level = level * jnp.repeat(steps, dims[axis_at] // shards_of).reshape([-1 if axis == axis_at else 1 for axis in range(len(dims))])
    return level


def noise(own_key, extent, scale, limit, pieces=(), held_as=jnp.bfloat16):
    entries = jax.random.normal(own_key, extent, jnp.float32) * scale
    if len(pieces) > 0:
        entries = level_of(own_key, extent, pieces, -0.22, 0.18) * entries
    return jnp.clip(entries, min=-limit, max=limit).astype(held_as)


def setup_inputs(seed: int = 0) -> dict:
    keys = jax.random.split(jax.random.key(seed), 6)
    field = noise(keys[0], (LAYERS, NODES, NODES, NODES, ER, NC), 1.0, 6.0, ((0, 4), (5, 32)), jnp.float32)
    coeffs = jnp.clip(jnp.exp(math.log(1.5) - 1.7917595 * jax.random.uniform(keys[1], (LAYERS, 3, NODES, NODES, NODES, ER, NC), jnp.float32) ** level_of(keys[1], (LAYERS, 3, NODES, NODES, NODES, ER, NC), ((0, 4), (6, 32)), -0.2, 0.2)), 0.25, 1.5)
    reaction = jnp.clip(jnp.exp(math.log(8.0) - 3.465736 * jax.random.uniform(keys[2], (LAYERS, NODES, NODES, NODES, ER, NC), jnp.float32) ** level_of(keys[2], (LAYERS, NODES, NODES, NODES, ER, NC), ((0, 4), (5, 32)), -0.2, 0.2)), 0.25, 8.0)
    step_scale = jnp.clip(jnp.exp(math.log(0.0003) - 1.09861236 * jax.random.uniform(keys[3], (LAYERS, NODES, NODES, NODES, ER, NC), jnp.float32) ** level_of(keys[3], (LAYERS, NODES, NODES, NODES, ER, NC), ((0, 4), (5, 32)), -0.2, 0.2)), 0.0001, 0.0003)
    rotation = plant(jax.random.randint(keys[4], (STEPS,), 0, NC * SUBSTEPS), jax.random.fold_in(keys[4], 1), 0, (NC * SUBSTEPS) - 1).astype(jnp.int32)
    return {"field": field, "coeffs": coeffs, "reaction": reaction, "step_scale": step_scale, "rotation": rotation}


def gll_points():
    return np.array([-1.0, -0.830223896278567, -0.4688487934707142, 0.0, 0.4688487934707142, 0.830223896278567, 1.0])


def derivative_table():
    points = gll_points()
    node_count = points.shape[0]
    weights = np.array([1.0 / np.prod([points[j] - points[k] for k in range(node_count) if k != j]) for j in range(node_count)])
    derivative = np.zeros((node_count, node_count))
    for i in range(node_count):
        for j in range(node_count):
            if i != j:
                derivative[i, j] = weights[j] / weights[i] / (points[i] - points[j])
        derivative[i, i] = -np.sum(derivative[i])
    return derivative


def lagrange_rows(locations):
    points = gll_points()
    identity_mask = np.eye(7) > 0.5
    differences = np.array([[1.0 if q == n else points[n] - points[q] for q in range(7)] for n in range(7)])
    denominator = np.prod(differences, axis=1)
    distances = locations[:, None] - jnp.asarray(points, jnp.float32)[None, :]
    factors = jnp.where(identity_mask[None, :, :], 1.0, distances[:, None, :])
    return jnp.prod(factors, axis=2) / jnp.asarray(denominator, jnp.float32)[None, :]


def mortar_tables(fraction):
    heights = (1.0 + jnp.asarray(gll_points(), jnp.float32)) * 0.5
    on_right = heights >= fraction
    shifted_height = jnp.where(on_right, heights - fraction, heights - fraction + 1.0)
    values = lagrange_rows(2.0 * shifted_height - 1.0)
    from_right = jnp.where(on_right[:, None], values, 0.0)
    from_left = jnp.where(on_right[:, None], 0.0, values)
    return from_left, from_right


def element_apply(field, coeffs, reaction):
    derivative = jnp.asarray(derivative_table(), jnp.float32)
    highest = lax.Precision.HIGHEST
    grad_axial = jnp.einsum("pa,arcxe->prcxe", derivative, field, precision=highest)
    grad_radial = jnp.einsum("pr,arcxe->apcxe", derivative, field, precision=highest)
    grad_circ = jnp.einsum("pc,arcxe->arpxe", derivative, field, precision=highest)
    result = reaction * field
    result = result + jnp.einsum("pa,prcxe->arcxe", derivative, coeffs[0] * grad_axial, precision=highest)
    result = result + jnp.einsum("pr,apcxe->arcxe", derivative, coeffs[1] * grad_radial, precision=highest)
    result = result + jnp.einsum("pc,arpxe->arcxe", derivative, coeffs[2] * grad_circ, precision=highest)
    return result


def layer_apply(inputs):
    return element_apply(inputs[0], inputs[1], inputs[2])


def reference(field, coeffs, reaction, step_scale, rotation):
    lower = LAYERS // 2 - 1
    highest = lax.Precision.HIGHEST
    current = field
    for step in range(STEPS):
        applied = lax.map(layer_apply, (current, coeffs, reaction))
        outer_faces = applied[:, :, 6]
        inner_faces = applied[:, :, 0]
        zero_row = jnp.zeros_like(inner_faces[:, :, :, :1])
        summed = applied.at[:, :, 6].add(jnp.concatenate([inner_faces[:, :, :, 1:], zero_row], axis=3))
        summed = summed.at[:, :, 0].add(jnp.concatenate([zero_row, outer_faces[:, :, :, :-1]], axis=3))
        summed = summed.at[:, :, :, 6].add(jnp.roll(applied[:, :, :, 0], -1, axis=4))
        summed = summed.at[:, :, :, 0].add(jnp.roll(applied[:, :, :, 6], 1, axis=4))
        top_faces = applied[:, 6]
        bottom_faces = applied[:, 0]
        offset = rotation[step]
        whole_k = (offset // SUBSTEPS).astype(jnp.int32)
        fraction = (offset % SUBSTEPS).astype(jnp.float32) / SUBSTEPS
        from_left, from_right = mortar_tables(fraction)
        rotor_top = top_faces[lower]
        stator_bottom = bottom_faces[lower + 1]
        stator_part = jnp.einsum("mn,rnxe->rmxe", from_left, jnp.roll(rotor_top, whole_k + 1, axis=3), precision=highest)
        stator_part = stator_part + jnp.einsum("mn,rnxe->rmxe", from_right, jnp.roll(rotor_top, whole_k, axis=3), precision=highest)
        rotor_part = jnp.einsum("mn,rmxe->rnxe", from_right, jnp.roll(stator_bottom, -whole_k, axis=3), precision=highest)
        rotor_part = rotor_part + jnp.einsum("mn,rmxe->rnxe", from_left, jnp.roll(stator_bottom, -whole_k - 1, axis=3), precision=highest)
        zero_face = jnp.zeros_like(top_faces[:1])
        from_below = jnp.concatenate([zero_face, top_faces[:-1]], axis=0)
        from_above = jnp.concatenate([bottom_faces[1:], zero_face], axis=0)
        from_below = from_below.at[lower + 1].set(stator_part)
        from_above = from_above.at[lower].set(rotor_part)
        summed = summed.at[:, 0].add(from_below)
        summed = summed.at[:, 6].add(from_above)
        current = current - step_scale * summed
    return current
```

```python
import jax
import jax.numpy as jnp
import numpy as np
from jax import lax
from jax.experimental import pallas as pl
from jax.experimental.pallas import tpu as pltpu
from jax.sharding import PartitionSpec as P

SUBSTEPS = 3
STEPS = 4
N = 7
CIRC = 32
SIDES = 4
VMEM_LIMIT = 16 * 2**20
AXES = ("circ", "side")


def gll_points():
    return np.array(
        [
            -1.0,
            -0.830223896278567,
            -0.4688487934707142,
            0.0,
            0.4688487934707142,
            0.830223896278567,
            1.0,
        ]
    )


def derivative_table():
    points = gll_points()
    weights = np.array(
        [1.0 / np.prod([points[j] - points[k] for k in range(N) if k != j]) for j in range(N)]
    )
    derivative = np.zeros((N, N))
    for i in range(N):
        for j in range(N):
            if i != j:
                derivative[i, j] = weights[j] / weights[i] / (points[i] - points[j])
        derivative[i, i] = -np.sum(derivative[i])
    return derivative


def mortar_table(substep):
    points = gll_points()
    heights = (1.0 + points) * 0.5
    fraction = substep / SUBSTEPS
    on_right = heights >= fraction
    local = 2.0 * np.where(on_right, heights - fraction, heights - fraction + 1.0) - 1.0
    table = np.array(
        [
            [
                np.prod([(at - points[q]) / (points[n] - points[q]) for q in range(N) if q != n])
                for n in range(N)
            ]
            for at in local
        ]
    )
    return table, ~on_right


D = derivative_table()
EVEN = [[float(0.5 * (D[p, q] + D[p, 6 - q])) for q in range(3)] for p in range(3)]
ODD = [[float(0.5 * (D[p, q] - D[p, 6 - q])) for q in range(3)] for p in range(3)]
TO_MID = [float(D[3, q]) for q in range(3)]
FROM_MID = [float(D[p, 3]) for p in range(3)]
TABLES = [mortar_table(substep) for substep in range(SUBSTEPS)]


def dot(weights, values):
    total = weights[0] * values[0]
    for weight, value in zip(weights[1:], values[1:]):
        total = total + weight * value
    return total


def differentiate(v):
    s = [v[i] + v[6 - i] for i in range(3)]
    d = [v[i] - v[6 - i] for i in range(3)]
    odd = [dot(EVEN[p] + [FROM_MID[p]], s + [v[3]]) for p in range(3)]
    even = [dot(ODD[p], d) for p in range(3)]
    mid = dot(TO_MID, d)
    return (
        [even[p] + odd[p] for p in range(3)] + [mid] + [even[p] - odd[p] for p in (2, 1, 0)]
    )


def differentiate_transposed(w):
    s = [w[i] + w[6 - i] for i in range(3)]
    d = [w[i] - w[6 - i] for i in range(3)]
    odd = [dot([ODD[p][q] for p in range(3)] + [TO_MID[q]], s + [w[3]]) for q in range(3)]
    even = [dot([EVEN[p][q] for p in range(3)], d) for q in range(3)]
    mid = dot(FROM_MID, d)
    return (
        [even[q] + odd[q] for q in range(3)] + [mid] + [even[q] - odd[q] for q in (2, 1, 0)]
    )


def along(coeffs, values):
    grad = differentiate(values)
    return differentiate_transposed([c * g for c, g in zip(coeffs, grad)])


def sparse_dot(weights, values):
    terms = [v if w == 1.0 else w * v for w, v in zip(weights, values) if w != 0.0]
    total = terms[0]
    for term in terms[1:]:
        total = total + term
    return total


def lanes():
    return lax.broadcasted_iota(jnp.int32, (8, 128), 1)


def rows():
    return lax.broadcasted_iota(jnp.int32, (8, 128), 0)


def upper_of(side):
    return jnp.where(side % 2 == 0, 6, 0)


def for_each_substep(condition, substep, run):
    for value in range(SUBSTEPS):

        @pl.when(condition & (substep == value))
        def _(value=value):
            table, left = TABLES[value]
            run(table, [int(is_left) for is_left in left])


def correct(info, step, scale, pair, mort_a, mort_b, circ_low, circ_high, u):
    side = info[8]
    within = info[step]
    substep = info[4 + step]
    upper = upper_of(side)
    lane = lanes()
    low = circ_low[...]
    high = circ_high[...]

    for a in range(N):
        for r in range(N):
            at = a * N + r
            from_low = jnp.where(lane == 0, pltpu.roll(low, (128 - at) % 128, 1), 0.0)
            from_high = jnp.where(lane == 127, pltpu.roll(high, 127 - at, 1), 0.0)
            u[a, r, 0] = u[a, r, 0] - scale[a, r, 0] * from_low
            u[a, r, 6] = u[a, r, 6] - scale[a, r, 6] * from_high

    def add_pair(r, _):
        for c in range(N):
            u[upper, r, c] = u[upper, r, c] - scale[upper, r, c] * pair[r, c]
        return 0

    lax.fori_loop(0, N, add_pair, 0)

    def to_stator(_, left):
        def add(r, _):
            for m in range(N):
                part = jnp.where(lane >= within + left[m], mort_a[r, m], mort_b[r, m])
                u[0, r, m] = u[0, r, m] - scale[0, r, m] * part
            return 0

        lax.fori_loop(0, N, add, 0)

    for_each_substep(side == 2, substep, to_stator)

    def to_rotor(table, left):
        def add(r, _):
            parts = [
                jnp.where(lane < 128 - within - left[m], mort_a[r, m], mort_b[r, m])
                for m in range(N)
            ]
            for n in range(N):
                part = sparse_dot([float(table[m, n]) for m in range(N)], parts)
                u[6, r, n] = u[6, r, n] - scale[6, r, n] * part
            return 0

        lax.fori_loop(0, N, add, 0)

    for_each_substep(side == 1, substep, to_rotor)


def apply_all(u, coeffs, reaction, acc, plane_ready, column_ready):
    def plane(a, _):
        plane_ready(a)
        for r in range(N):
            values = [u[a, r, c] for c in range(N)]
            out = along([coeffs[2, a, r, c] for c in range(N)], values)
            for c in range(N):
                acc[a, r, c] = out[c] + reaction[a, r, c] * values[c]
        for c in range(N):
            out = along(
                [coeffs[1, a, r, c] for r in range(N)], [u[a, r, c] for r in range(N)]
            )
            for r in range(N):
                acc[a, r, c] = acc[a, r, c] + out[r]
        return 0

    lax.fori_loop(0, N, plane, 0)
    column_ready()

    def column(r, _):
        for c in range(N):
            out = along(
                [coeffs[0, a, r, c] for a in range(N)], [u[a, r, c] for a in range(N)]
            )
            for a in range(N):
                acc[a, r, c] = acc[a, r, c] + out[a]
        return 0

    lax.fori_loop(0, N, column, 0)


def send_faces(info, step, acc, pair, mort):
    side = info[8]
    within = info[step]
    substep = info[4 + step]
    upper = upper_of(side)

    def pair_row(r, _):
        for c in range(N):
            pair[r, c] = acc[upper, r, c]
        return 0

    lax.fori_loop(0, N, pair_row, 0)

    def from_rotor(table, left):
        def row(r, _):
            values = [acc[6, r, n] for n in range(N)]
            for m in range(N):
                part = sparse_dot([float(x) for x in table[m]], values)
                mort[r, m] = pltpu.roll(part, (within + left[m]) % 128, 1)
            return 0

        lax.fori_loop(0, N, row, 0)

    for_each_substep(side == 1, substep, from_rotor)

    def from_stator(_, left):
        def row(r, _):
            for m in range(N):
                mort[r, m] = pltpu.roll(acc[0, r, m], (128 - within - left[m]) % 128, 1)
            return 0

        lax.fori_loop(0, N, row, 0)

    for_each_substep(side == 2, substep, from_stator)


def update(u, scale, acc, u_out, to_high, to_low):
    lane = lanes()
    row = rows()

    def layer(a, carry):
        high, low = carry
        for r in range(N):
            inner = acc[a, r, 0]
            outer = acc[a, r, 6]
            for c in range(N):
                total = acc[a, r, c]
                if c == 0:
                    total = total + jnp.where(lane == 0, 0.0, pltpu.roll(outer, 1, 1))
                if c == 6:
                    total = total + jnp.where(lane == 127, 0.0, pltpu.roll(inner, 127, 1))
                if r == 0:
                    total = total + jnp.where(row == 0, 0.0, pltpu.roll(acc[a, 6, c], 1, 0))
                if r == 6:
                    total = total + jnp.where(row == 7, 0.0, pltpu.roll(acc[a, 0, c], 7, 0))
                u_out[a, r, c] = u[a, r, c] - scale[a, r, c] * total
            at = a * N + r
            high = jnp.where(lane == at, pltpu.roll(outer, at + 1, 1), high)
            low = jnp.where(lane == at, pltpu.roll(inner, at, 1), low)
        return high, low

    zero = jnp.zeros((8, 128), jnp.float32)
    high, low = lax.fori_loop(0, N, layer, (zero, zero))
    to_high[...] = high
    to_low[...] = low


def start_loads(coeffs, reaction, coeffs_v, reaction_v, sems):
    def plane_copies(a):
        return [
            pltpu.make_async_copy(coeffs.at[2, a], coeffs_v.at[2, a], sems.at[a]),
            pltpu.make_async_copy(coeffs.at[1, a], coeffs_v.at[1, a], sems.at[7 + a]),
            pltpu.make_async_copy(reaction.at[a], reaction_v.at[a], sems.at[14 + a]),
        ]

    column_copy = pltpu.make_async_copy(coeffs.at[0], coeffs_v.at[0], sems.at[21])
    for a in range(N):
        for copy in plane_copies(a):
            copy.start()
    column_copy.start()

    def plane_ready(a):
        for copy in plane_copies(a):
            copy.wait()

    return plane_ready, column_copy.wait


def first_kernel(
    info, field, coeffs, reaction, scale,
    u_out, pair, mort, to_high, to_low, u, acc, coeffs_v, reaction_v, scale_v, sems,
):
    field_copies = [pltpu.make_async_copy(field.at[a], u.at[a], sems.at[23 + a]) for a in range(N)]
    scale_copy = pltpu.make_async_copy(scale, scale_v, sems.at[22])
    for copy in field_copies:
        copy.start()
    plane_ready, column_ready = start_loads(coeffs, reaction, coeffs_v, reaction_v, sems)
    scale_copy.start()
    for copy in field_copies:
        copy.wait()
    apply_all(u, coeffs_v, reaction_v, acc, plane_ready, column_ready)
    send_faces(info, 0, acc, pair, mort)
    scale_copy.wait()
    update(u, scale_v, acc, u_out, to_high, to_low)


def step_kernel(
    info, at_step, u, coeffs, reaction, scale, pair_in, mort_a, mort_b, low_in, high_in,
    u_out, pair, mort, to_high, to_low, acc, coeffs_v, reaction_v, scale_v, sems,
):
    step = at_step[0]
    more = step < STEPS - 1
    scale_copy = pltpu.make_async_copy(scale, scale_v, sems.at[22])
    scale_copy.start()

    @pl.when(more)
    def _():
        start_loads(coeffs, reaction, coeffs_v, reaction_v, sems)

    scale_copy.wait()
    correct(info, step, scale_v, pair_in, mort_a, mort_b, low_in, high_in, u)

    @pl.when(more)
    def _():
        def plane_ready(a):
            for source, target, sem in (
                (coeffs.at[2, a], coeffs_v.at[2, a], sems.at[a]),
                (coeffs.at[1, a], coeffs_v.at[1, a], sems.at[7 + a]),
                (reaction.at[a], reaction_v.at[a], sems.at[14 + a]),
            ):
                pltpu.make_async_copy(source, target, sem).wait()

        column_copy = pltpu.make_async_copy(coeffs.at[0], coeffs_v.at[0], sems.at[21])
        apply_all(u, coeffs_v, reaction_v, acc, plane_ready, column_copy.wait)
        send_faces(info, step + 1, acc, pair, mort)
        update(u, scale_v, acc, u_out, to_high, to_low)

    @pl.when(step == STEPS - 1)
    def _():
        def copy(a, _):
            for r in range(N):
                for c in range(N):
                    u_out[a, r, c] = u[a, r, c]
            return 0

        lax.fori_loop(0, N, copy, 0)


def at(circ, side):
    return (circ % CIRC) * SIDES + side


PAIR = [(at(c, s), at(c, s ^ 1)) for c in range(CIRC) for s in range(SIDES)]
UP = [(at(c, s), at(c + 1, s)) for c in range(CIRC) for s in range(SIDES)]
DOWN = [(at(c, s), at(c - 1, s)) for c in range(CIRC) for s in range(SIDES)]


def rotated(hops):
    pairs = []
    for c in range(CIRC):
        pairs.append((at(c, 1), at(c + hops, 2)))
        pairs.append((at(c, 2), at(c - hops, 1)))
    return pairs


def exchange(hops, mort):
    return lax.ppermute(mort, AXES, rotated(hops)), lax.ppermute(mort, AXES, rotated(hops + 1))


def local(field, coeffs, reaction, step_scale, rotation):
    field, coeffs, reaction, step_scale = field[0], coeffs[0], reaction[0], step_scale[0]
    whole_k = rotation // SUBSTEPS
    sector = whole_k // 128
    side = lax.axis_index("side").astype(jnp.int32)
    info = jnp.concatenate([whole_k % 128, rotation % SUBSTEPS, side[None]])
    like = lambda x: pltpu.VMEM(x.shape, jnp.float32)
    face = jax.ShapeDtypeStruct(field.shape[1:], jnp.float32)
    edge = jax.ShapeDtypeStruct((8, 128), jnp.float32)
    sends = (like(field), face, face, edge, edge)
    vmem = pl.BlockSpec(memory_space=pltpu.VMEM)
    smem = pl.BlockSpec(memory_space=pltpu.SMEM)
    hbm = pl.BlockSpec(memory_space=pltpu.HBM)
    scratch = pltpu.VMEM(field.shape, jnp.float32)
    params = pltpu.CompilerParams(vmem_limit_bytes=VMEM_LIMIT)
    branches = [lambda mort, hops=hops: exchange(hops, mort) for hops in range(CIRC)]
    field, *fixed = [
        pltpu.with_memory_space_constraint(x, pltpu.HBM)
        for x in (field, coeffs, reaction, step_scale)
    ]
    buffers = [scratch, pltpu.VMEM(coeffs.shape, jnp.float32), scratch, scratch]
    carry = pl.pallas_call(
        first_kernel,
        out_shape=sends,
        in_specs=[smem] + [hbm] * 4,
        out_specs=(vmem,) * 5,
        scratch_shapes=[scratch] + buffers + [pltpu.SemaphoreType.DMA((30,))],
        compiler_params=params,
        name="first",
    )(info, field, *fixed)
    advance = pl.pallas_call(
        step_kernel,
        out_shape=sends,
        in_specs=[smem, smem, vmem] + [hbm] * 3 + [vmem] * 5,
        out_specs=(vmem,) * 5,
        scratch_shapes=buffers + [pltpu.SemaphoreType.DMA((23,))],
        input_output_aliases={2: 0},
        compiler_params=params,
        name="step",
    )

    def body(step, carry):
        u, pair, mort, to_high, to_low = carry
        low = lax.ppermute(to_high, AXES, UP)
        high = lax.ppermute(to_low, AXES, DOWN)
        pair = lax.ppermute(pair, AXES, PAIR)
        mort_a, mort_b = lax.switch(sector[step], branches, mort)
        kept = [pltpu.with_memory_space_constraint(x, pltpu.HBM) for x in fixed]
        return advance(info, step[None], u, *kept, pair, mort_a, mort_b, low, high)

    return lax.fori_loop(0, STEPS, body, carry)[0][None]


def solution(mesh):
    in_specs = (
        P("side", None, None, None, None, "circ"),
        P("side", None, None, None, None, None, "circ"),
        P("side", None, None, None, None, "circ"),
        P("side", None, None, None, None, "circ"),
        P(),
    )
    out_specs = P("side", None, None, None, None, "circ")
    return jax.shard_map(local, mesh=mesh, in_specs=in_specs, out_specs=out_specs, check_vma=False)
```

```python
import jax
import jax.numpy as jnp
import numpy as np
from jax import lax
from jax.experimental import pallas as pl
from jax.experimental.pallas import tpu as pltpu
from jax.sharding import PartitionSpec as P

SUBSTEPS = 3
STEPS = 4
N = 7
CIRC = 32
SIDES = 4
VMEM_LIMIT = 16 * 2**20
AXES = ("circ", "side")


def gll_points():
    return np.array(
        [
            -1.0,
            -0.830223896278567,
            -0.4688487934707142,
            0.0,
            0.4688487934707142,
            0.830223896278567,
            1.0,
        ]
    )


def derivative_table():
    points = gll_points()
    weights = np.array(
        [1.0 / np.prod([points[j] - points[k] for k in range(N) if k != j]) for j in range(N)]
    )
    derivative = np.zeros((N, N))
    for i in range(N):
        for j in range(N):
            if i != j:
                derivative[i, j] = weights[j] / weights[i] / (points[i] - points[j])
        derivative[i, i] = -np.sum(derivative[i])
    return derivative


def mortar_table(substep):
    points = gll_points()
    heights = (1.0 + points) * 0.5
    fraction = substep / SUBSTEPS
    on_right = heights >= fraction
    local = 2.0 * np.where(on_right, heights - fraction, heights - fraction + 1.0) - 1.0
    table = np.array(
        [
            [
                np.prod([(at - points[q]) / (points[n] - points[q]) for q in range(N) if q != n])
                for n in range(N)
            ]
            for at in local
        ]
    )
    return table, ~on_right


D = derivative_table()
EVEN = [[float(0.5 * (D[p, q] + D[p, 6 - q])) for q in range(3)] for p in range(3)]
ODD = [[float(0.5 * (D[p, q] - D[p, 6 - q])) for q in range(3)] for p in range(3)]
TO_MID = [float(D[3, q]) for q in range(3)]
FROM_MID = [float(D[p, 3]) for p in range(3)]
TABLES = [mortar_table(substep) for substep in range(SUBSTEPS)]


def dot(weights, values):
    total = weights[0] * values[0]
    for weight, value in zip(weights[1:], values[1:]):
        total = total + weight * value
    return total


def differentiate(v):
    s = [v[i] + v[6 - i] for i in range(3)]
    d = [v[i] - v[6 - i] for i in range(3)]
    odd = [dot(EVEN[p] + [FROM_MID[p]], s + [v[3]]) for p in range(3)]
    even = [dot(ODD[p], d) for p in range(3)]
    mid = dot(TO_MID, d)
    return (
        [even[p] + odd[p] for p in range(3)] + [mid] + [even[p] - odd[p] for p in (2, 1, 0)]
    )


def differentiate_transposed(w):
    s = [w[i] + w[6 - i] for i in range(3)]
    d = [w[i] - w[6 - i] for i in range(3)]
    odd = [dot([ODD[p][q] for p in range(3)] + [TO_MID[q]], s + [w[3]]) for q in range(3)]
    even = [dot([EVEN[p][q] for p in range(3)], d) for q in range(3)]
    mid = dot(FROM_MID, d)
    return (
        [even[q] + odd[q] for q in range(3)] + [mid] + [even[q] - odd[q] for q in (2, 1, 0)]
    )


def along(coeffs, values):
    grad = differentiate(values)
    return differentiate_transposed([c * g for c, g in zip(coeffs, grad)])


def sparse_dot(weights, values):
    terms = [v if w == 1.0 else w * v for w, v in zip(weights, values) if w != 0.0]
    total = terms[0]
    for term in terms[1:]:
        total = total + term
    return total


def lanes():
    return lax.broadcasted_iota(jnp.int32, (8, 128), 1)


def rows():
    return lax.broadcasted_iota(jnp.int32, (8, 128), 0)


def upper_of(side):
    return jnp.where(side % 2 == 0, 6, 0)


def for_each_substep(condition, substep, run):
    for value in range(SUBSTEPS):

        @pl.when(condition & (substep == value))
        def _(value=value):
            table, left = TABLES[value]
            run(table, [int(is_left) for is_left in left])


def copy_and_correct_edges(info, scale, first, second, u_in, u):
    lane = lanes()
    even = info[9] == 0
    high = jnp.where(even, first[...], second[...])
    low = jnp.where(even, second[...], first[...])
    for a in range(N):
        for r in range(N):
            at = a * N + r
            from_low = jnp.where(lane == 0, pltpu.roll(low, (128 - at) % 128, 1), 0.0)
            from_high = jnp.where(lane == 127, pltpu.roll(high, 127 - at, 1), 0.0)
            for c in range(1, 6):
                u[a, r, c] = u_in[a, r, c]
            u[a, r, 0] = u_in[a, r, 0] - scale[a, r, 0] * from_low
            u[a, r, 6] = u_in[a, r, 6] - scale[a, r, 6] * from_high


def left_count(substep):
    counts = [int(left.sum()) for _, left in TABLES]
    return jnp.where(substep == 0, counts[0], jnp.where(substep == 1, counts[1], counts[2]))


def correct_faces(info, step, scale, pair, big, small, u):
    side = info[8]
    within = info[step]
    substep = info[4 + step]
    upper = upper_of(side)
    lane = lanes()
    for r in range(N):
        for c in range(N):
            u[upper, r, c] = u[upper, r, c] - scale[upper, r, c] * pair[r, c]

    @pl.when((side == 1) | (side == 2))
    def _():
        low = (within < 64) == (side == 2)
        place = jnp.where(low, lane, 127 - lane)
        turns = [jnp.where(low, 0, 64), jnp.where(low, 64, 0)]
        lefts = left_count(substep)
        limits = []
        for m in range(N):
            moved = within + jnp.where(m < lefts, 1, 0)
            first = jnp.where(side == 2, moved, 128 - moved)
            limits.append(jnp.where(low, first, 128 - first))
        for at in range(N * N):
            half = pltpu.roll(small[at // 2], turns[at % 2], 1)
            big[at] = jnp.where(place < limits[at % N], half, big[at])

    @pl.when(side == 2)
    def _():
        for r in range(N):
            for m in range(N):
                u[0, r, m] = u[0, r, m] - scale[0, r, m] * big[r * N + m]

    def to_rotor(table, _):
        def add(r, _):
            parts = [big[r * N + m] for m in range(N)]
            for n in range(N):
                part = sparse_dot([float(table[m, n]) for m in range(N)], parts)
                u[6, r, n] = u[6, r, n] - scale[6, r, n] * part
            return 0

        lax.fori_loop(0, N, add, 0)

    for_each_substep(side == 1, substep, to_rotor)


def apply_all(u, coeffs, reaction, acc, plane_ready, column_ready):
    def plane(i, _):
        a = lax.rem(i + 1, N)
        plane_ready(i, a)
        for r in range(N):
            values = [u[a, r, c] for c in range(N)]
            out = along([coeffs[2, a, r, c] for c in range(N)], values)
            for c in range(N):
                acc[a, r, c] = out[c] + reaction[a, r, c] * values[c]
        for c in range(N):
            out = along(
                [coeffs[1, a, r, c] for r in range(N)], [u[a, r, c] for r in range(N)]
            )
            for r in range(N):
                acc[a, r, c] = acc[a, r, c] + out[r]
        return 0

    lax.fori_loop(0, N, plane, 0)
    column_ready()

    def column(r, _):
        for c in range(N):
            out = along(
                [coeffs[0, a, r, c] for a in range(N)], [u[a, r, c] for a in range(N)]
            )
            for a in range(N):
                acc[a, r, c] = acc[a, r, c] + out[a]
        return 0

    lax.fori_loop(0, N, column, 0)


def send_faces(info, step, acc, pair, big, small, face):
    side = info[8]
    within = info[step]
    substep = info[4 + step]
    upper = upper_of(side)
    lane = lanes()
    for r in range(N):
        for c in range(N):
            pair[r, c] = acc[upper, r, c]

    def from_rotor(table, _):
        def row(r, _):
            values = [acc[6, r, n] for n in range(N)]
            for m in range(N):
                face[r * N + m] = sparse_dot([float(x) for x in table[m]], values)
            return 0

        lax.fori_loop(0, N, row, 0)

    for_each_substep(side == 1, substep, from_rotor)

    @pl.when(side == 2)
    def _():
        for r in range(N):
            for m in range(N):
                face[r * N + m] = acc[0, r, m]

    @pl.when((side == 1) | (side == 2))
    def _():
        lefts = left_count(substep)
        shifts = []
        for m in range(N):
            moved = within + jnp.where(m < lefts, 1, 0)
            shifts.append(jnp.where(side == 1, moved, 128 - moved))
        half = jnp.where((within < 64) == (side == 1), 0, 64)
        for at in range(N * N):
            big[at] = pltpu.roll(face[at], lax.rem(shifts[at % N], 128), 1)
        for g in range((N * N + 1) // 2):
            first = pltpu.roll(face[2 * g], lax.rem(shifts[2 * g % N] + half, 128), 1)
            at = min(2 * g + 1, N * N - 1)
            second = pltpu.roll(face[at], lax.rem(shifts[at % N] + 64 + half, 128), 1)
            small[g] = jnp.where(lane < 64, first, second)


def update(info, u, scale, acc, u_out, edge_first, edge_second):
    lane = lanes()
    row = rows()

    def layer(a, carry):
        high, low = carry
        for r in range(N):
            inner = acc[a, r, 0]
            outer = acc[a, r, 6]
            for c in range(N):
                total = acc[a, r, c]
                if c == 0:
                    total = total + jnp.where(lane == 0, 0.0, pltpu.roll(outer, 1, 1))
                if c == 6:
                    total = total + jnp.where(lane == 127, 0.0, pltpu.roll(inner, 127, 1))
                if r == 0:
                    total = total + jnp.where(row == 0, 0.0, pltpu.roll(acc[a, 6, c], 1, 0))
                if r == 6:
                    total = total + jnp.where(row == 7, 0.0, pltpu.roll(acc[a, 0, c], 7, 0))
                u_out[a, r, c] = u[a, r, c] - scale[a, r, c] * total
            at = a * N + r
            high = jnp.where(lane == at, pltpu.roll(outer, at + 1, 1), high)
            low = jnp.where(lane == at, pltpu.roll(inner, at, 1), low)
        return high, low

    zero = jnp.zeros((8, 128), jnp.float32)
    high, low = lax.fori_loop(0, N, layer, (zero, zero))
    even = info[9] == 0
    edge_first[...] = jnp.where(even, high, low)
    edge_second[...] = jnp.where(even, low, high)


def loads(coeffs, reaction, coeffs_v, reaction_v, sems):
    def plane_copies(a):
        return [
            pltpu.make_async_copy(coeffs.at[2, a], coeffs_v.at[2, a], sems.at[a]),
            pltpu.make_async_copy(coeffs.at[1, a], coeffs_v.at[1, a], sems.at[7 + a]),
            pltpu.make_async_copy(reaction.at[a], reaction_v.at[a], sems.at[14 + a]),
        ]

    return plane_copies, pltpu.make_async_copy(coeffs.at[0], coeffs_v.at[0], sems.at[21])


def first_kernel(
    info, field, coeffs, reaction, scale,
    u_out, pair, big, small, edge_first, edge_second, scale_v,
    acc, coeffs_v, reaction_v, u, face, sems,
):
    plane_copies, column_copy = loads(coeffs, reaction, coeffs_v, reaction_v, sems)
    field_copies = [pltpu.make_async_copy(field.at[a], u.at[a], sems.at[23 + a]) for a in range(N)]
    scale_copy = pltpu.make_async_copy(scale, scale_v, sems.at[22])
    for i in range(N):
        a = (i + 1) % N
        field_copies[a].start()
        for copy in plane_copies(a):
            copy.start()
    column_copy.start()
    scale_copy.start()

    def plane_ready(i, a):
        pltpu.make_async_copy(field.at[a], u.at[a], sems.at[23 + a]).wait()
        for copy in plane_copies(a):
            copy.wait()

    apply_all(u, coeffs_v, reaction_v, acc, plane_ready, column_copy.wait)
    send_faces(info, 0, acc, pair, big, small, face)
    scale_copy.wait()
    update(info, u, scale_v, acc, u_out, edge_first, edge_second)


def step_kernel(
    info, at_step, u_in, scale, coeffs, reaction, pair_in, big_in, small_in, first_in, second_in,
    u_out, pair, big, small, edge_first, edge_second, _scale,
    acc, coeffs_v, reaction_v, u, big_v, small_v, sems,
):
    step = at_step[0]
    more = step < STEPS - 1
    plane_copies, column_copy = loads(coeffs, reaction, coeffs_v, reaction_v, sems)
    big_copy = pltpu.make_async_copy(big_in, big_v, sems.at[22])
    small_copy = pltpu.make_async_copy(small_in, small_v, sems.at[23])

    @pl.when(more)
    def _():
        for i in range(N):
            for copy in plane_copies((i + 1) % N):
                copy.start()
            if i == 2:
                big_copy.start()
                small_copy.start()
        column_copy.start()

    def faces():
        big_copy.wait()
        small_copy.wait()
        correct_faces(info, step, scale, pair_in, big_v, small_v, u)

    copy_and_correct_edges(info, scale, first_in, second_in, u_in, u)

    @pl.when(more)
    def _():
        def plane_ready(i, a):
            for copy in plane_copies(a):
                copy.wait()

            @pl.when(i == N - 2)
            def _():
                faces()

        apply_all(u, coeffs_v, reaction_v, acc, plane_ready, column_copy.wait)
        send_faces(info, step + 1, acc, pair, big, small, big_v)
        update(info, u, scale, acc, u_out, edge_first, edge_second)

    @pl.when(step == STEPS - 1)
    def _():
        big_copy.start()
        small_copy.start()
        faces()

        def copy(a, _):
            for r in range(N):
                for c in range(N):
                    u_out[a, r, c] = u[a, r, c]
            return 0

        lax.fori_loop(0, N, copy, 0)


def at(circ, side):
    return (circ % CIRC) * SIDES + side


EVERY = [(c, s) for c in range(CIRC) for s in range(SIDES)]
PAIR = [(at(c, s), at(c, s ^ 1)) for c, s in EVERY]
SWAP_FIRST = [(at(c, s), at(c ^ 1, s)) for c, s in EVERY]
SWAP_SECOND = [(at(c, s), at(c + (1 if c % 2 else -1), s)) for c, s in EVERY]


def rotated(hops):
    pairs = []
    for c in range(CIRC):
        pairs.append((at(c, 1), at(c + hops, 2)))
        pairs.append((at(c, 2), at(c - hops, 1)))
    return pairs


def exchange(big_hops, small_hops, big, small):
    big = lax.ppermute(big, AXES, rotated(big_hops))
    return big, lax.ppermute(small, AXES, rotated(small_hops))


def local(field, coeffs, reaction, step_scale, rotation):
    field, coeffs, reaction, step_scale = field[0], coeffs[0], reaction[0], step_scale[0]
    whole_k = rotation // SUBSTEPS
    within = whole_k % 128
    branch = whole_k // 128 + jnp.where(within < 64, 0, CIRC)
    branches = [lambda *v, h=h: exchange(h, h + 1, *v) for h in range(CIRC)]
    branches += [lambda *v, h=h: exchange(h + 1, h, *v) for h in range(CIRC)]
    side = lax.axis_index("side").astype(jnp.int32)
    parity = lax.axis_index("circ").astype(jnp.int32) % 2
    info = jnp.concatenate([within, rotation % SUBSTEPS, side[None], parity[None]])

    array = lambda *shape: jax.ShapeDtypeStruct(shape, jnp.float32)
    node = pltpu.VMEM(field.shape, jnp.float32)
    face, edge = array(*field.shape[1:]), array(8, 128)
    sends = (node, face, array(49, 8, 128), array(25, 8, 128), edge, edge, node)
    vmem = pl.BlockSpec(memory_space=pltpu.VMEM)
    smem = pl.BlockSpec(memory_space=pltpu.SMEM)
    hbm = pl.BlockSpec(memory_space=pltpu.HBM)
    buffers = [pltpu.VMEM(shape, jnp.float32) for shape in (field.shape, coeffs.shape, field.shape)]
    bigger = pltpu.VMEM((49, 8, 128), jnp.float32)
    params = pltpu.CompilerParams(vmem_limit_bytes=VMEM_LIMIT)
    field, coeffs, reaction, step_scale = [
        pltpu.with_memory_space_constraint(x, pltpu.HBM)
        for x in (field, coeffs, reaction, step_scale)
    ]
    carry = pl.pallas_call(
        first_kernel,
        out_shape=sends,
        in_specs=[smem] + [hbm] * 4,
        out_specs=(vmem,) * 7,
        scratch_shapes=buffers + [buffers[0], bigger, pltpu.SemaphoreType.DMA((30,))],
        compiler_params=params,
        name="first",
    )(info, field, coeffs, reaction, step_scale)
    advance = pl.pallas_call(
        step_kernel,
        out_shape=sends,
        in_specs=[smem, smem, vmem, vmem, hbm, hbm, vmem, hbm, hbm, vmem, vmem],
        out_specs=(vmem,) * 7,
        scratch_shapes=buffers
        + [buffers[0], bigger, pltpu.VMEM((25, 8, 128), jnp.float32)]
        + [pltpu.SemaphoreType.DMA((24,))],
        input_output_aliases={2: 0, 3: 6},
        compiler_params=params,
        name="step",
    )

    def body(step, carry):
        u, pair, big, small, edge_first, edge_second, scale = carry
        pair = lax.ppermute(pair, AXES, PAIR)
        first = lax.ppermute(edge_first, AXES, SWAP_FIRST)
        second = lax.ppermute(edge_second, AXES, SWAP_SECOND)
        big, small = lax.switch(branch[step], branches, big, small)
        streamed = [pltpu.with_memory_space_constraint(x, pltpu.HBM) for x in (coeffs, reaction)]
        return advance(
            info, step[None], u, scale, *streamed, pair, big, small, first, second
        )

    return lax.fori_loop(0, STEPS, body, tuple(carry))[0][None]


def solution(mesh):
    in_specs = (
        P("side", None, None, None, None, "circ"),
        P("side", None, None, None, None, None, "circ"),
        P("side", None, None, None, None, "circ"),
        P("side", None, None, None, None, "circ"),
        P(),
    )
    out_specs = P("side", None, None, None, None, "circ")
    return jax.shard_map(local, mesh=mesh, in_specs=in_specs, out_specs=out_specs, check_vma=False)
```

```python
from typing import NamedTuple

import jax
import jax.numpy as jnp
import numpy as np
from jax import lax
from jax.experimental import pallas as pl
from jax.experimental.pallas import tpu as pltpu
from jax.sharding import PartitionSpec as P

SUBSTEPS = 3
STEPS = 4
N = 7
CIRC = 32
SIDES = 4
VMEM_LIMIT = 16 * 2**20
AXES = ("circ", "side")


def gll_points():
    return np.array(
        [
            -1.0,
            -0.830223896278567,
            -0.4688487934707142,
            0.0,
            0.4688487934707142,
            0.830223896278567,
            1.0,
        ]
    )


def derivative_table():
    points = gll_points()
    weights = np.array(
        [1.0 / np.prod([points[j] - points[k] for k in range(N) if k != j]) for j in range(N)]
    )
    derivative = np.zeros((N, N))
    for i in range(N):
        for j in range(N):
            if i != j:
                derivative[i, j] = weights[j] / weights[i] / (points[i] - points[j])
        derivative[i, i] = -np.sum(derivative[i])
    return derivative


def mortar_table(substep):
    points = gll_points()
    heights = (1.0 + points) * 0.5
    fraction = substep / SUBSTEPS
    on_right = heights >= fraction
    local = 2.0 * np.where(on_right, heights - fraction, heights - fraction + 1.0) - 1.0
    table = np.array(
        [
            [
                np.prod([(at - points[q]) / (points[n] - points[q]) for q in range(N) if q != n])
                for n in range(N)
            ]
            for at in local
        ]
    )
    return table, ~on_right


D = derivative_table()
EVEN = [[float(0.5 * (D[p, q] + D[p, 6 - q])) for q in range(3)] for p in range(3)]
ODD = [[float(0.5 * (D[p, q] - D[p, 6 - q])) for q in range(3)] for p in range(3)]
TO_MID = [float(D[3, q]) for q in range(3)]
FROM_MID = [float(D[p, 3]) for p in range(3)]
TABLES = [mortar_table(substep) for substep in range(SUBSTEPS)]


def dot(weights, values):
    total = weights[0] * values[0]
    for weight, value in zip(weights[1:], values[1:]):
        total = total + weight * value
    return total


def differentiate(v):
    s = [v[i] + v[6 - i] for i in range(3)]
    d = [v[i] - v[6 - i] for i in range(3)]
    odd = [dot(EVEN[p] + [FROM_MID[p]], s + [v[3]]) for p in range(3)]
    even = [dot(ODD[p], d) for p in range(3)]
    mid = dot(TO_MID, d)
    return (
        [even[p] + odd[p] for p in range(3)] + [mid] + [even[p] - odd[p] for p in (2, 1, 0)]
    )


def differentiate_transposed(w):
    s = [w[i] + w[6 - i] for i in range(3)]
    d = [w[i] - w[6 - i] for i in range(3)]
    odd = [dot([ODD[p][q] for p in range(3)] + [TO_MID[q]], s + [w[3]]) for q in range(3)]
    even = [dot([EVEN[p][q] for p in range(3)], d) for q in range(3)]
    mid = dot(FROM_MID, d)
    return (
        [even[q] + odd[q] for q in range(3)] + [mid] + [even[q] - odd[q] for q in (2, 1, 0)]
    )


def along(coeffs, values):
    grad = differentiate(values)
    return differentiate_transposed([c * g for c, g in zip(coeffs, grad)])


def sparse_dot(weights, values):
    terms = [v if w == 1.0 else w * v for w, v in zip(weights, values) if w != 0.0]
    total = terms[0]
    for term in terms[1:]:
        total = total + term
    return total


def lanes():
    return lax.broadcasted_iota(jnp.int32, (8, 128), 1)


def rows():
    return lax.broadcasted_iota(jnp.int32, (8, 128), 0)


class Place(NamedTuple):
    side: jax.Array
    even: jax.Array
    sector: jax.Array
    within: jax.Array
    substep: jax.Array


def place_at(rotation, step):
    whole = lax.div(rotation[step], SUBSTEPS)
    return Place(
        side=lax.axis_index("side"),
        even=lax.rem(lax.axis_index("circ"), 2) == 0,
        sector=lax.div(whole, 128),
        within=lax.rem(whole, 128),
        substep=rotation[step] - SUBSTEPS * whole,
    )


def branch_of(place):
    return place.sector + jnp.where(place.within < 64, 0, CIRC)


def upper_of(side):
    return jnp.where(side % 2 == 0, 6, 0)


def for_each_substep(condition, substep, run):
    for value in range(SUBSTEPS):

        @pl.when(condition & (substep == value))
        def _(value=value):
            table, left = TABLES[value]
            run(table, [int(is_left) for is_left in left])


def copy_and_correct_edges(place, scale, edges, u_in, u):
    lane = lanes()
    first, second = [edge[...] for edge in edges]
    high = jnp.where(place.even, first, second)
    low = jnp.where(place.even, second, first)
    for a in range(N):
        for r in range(N):
            at = a * N + r
            from_low = jnp.where(lane == 0, pltpu.roll(low, (128 - at) % 128, 1), 0.0)
            from_high = jnp.where(lane == 127, pltpu.roll(high, 127 - at, 1), 0.0)
            for c in range(1, 6):
                u[a, r, c] = u_in[a, r, c]
            u[a, r, 0] = u_in[a, r, 0] - scale[a, r, 0] * from_low
            u[a, r, 6] = u_in[a, r, 6] - scale[a, r, 6] * from_high


def left_count(substep):
    counts = [int(left.sum()) for _, left in TABLES]
    return jnp.where(substep == 0, counts[0], jnp.where(substep == 1, counts[1], counts[2]))


def correct_faces(where, scale, pair, big, small, u):
    side, within, substep = where.side, where.within, where.substep
    upper = upper_of(side)
    lane = lanes()
    for r in range(N):
        for c in range(N):
            u[upper, r, c] = u[upper, r, c] - scale[upper, r, c] * pair[r, c]

    @pl.when((side == 1) | (side == 2))
    def _():
        low = (within < 64) == (side == 2)
        place = jnp.where(low, lane, 127 - lane)
        turns = [jnp.where(low, 0, 64), jnp.where(low, 64, 0)]
        lefts = left_count(substep)
        limits = []
        for m in range(N):
            moved = within + jnp.where(m < lefts, 1, 0)
            first = jnp.where(side == 2, moved, 128 - moved)
            limits.append(jnp.where(low, first, 128 - first))
        for at in range(N * N):
            half = pltpu.roll(small[at // 2], turns[at % 2], 1)
            big[at] = jnp.where(place < limits[at % N], half, big[at])

    @pl.when(side == 2)
    def _():
        for r in range(N):
            for m in range(N):
                u[0, r, m] = u[0, r, m] - scale[0, r, m] * big[r * N + m]

    def to_rotor(table, _):
        def add(r, _):
            parts = [big[r * N + m] for m in range(N)]
            for n in range(N):
                part = sparse_dot([float(table[m, n]) for m in range(N)], parts)
                u[6, r, n] = u[6, r, n] - scale[6, r, n] * part
            return 0

        lax.fori_loop(0, N, add, 0)

    for_each_substep(side == 1, substep, to_rotor)


def apply_planes(u, coeffs, reaction, acc, plane_ready):
    def plane(i, _):
        a = lax.rem(i + 1, N)
        plane_ready(i, a)
        for r in range(N):
            values = [u[a, r, c] for c in range(N)]
            out = along([coeffs[2, a, r, c] for c in range(N)], values)
            for c in range(N):
                acc[a, r, c] = out[c] + reaction[a, r, c] * values[c]
        for c in range(N):
            out = along(
                [coeffs[1, a, r, c] for r in range(N)], [u[a, r, c] for r in range(N)]
            )
            for r in range(N):
                acc[a, r, c] = acc[a, r, c] + out[r]
        return 0

    lax.fori_loop(0, N, plane, 0)


def finish(where, u, coeffs, scale, acc, u_out, edge_first, edge_second, column_ready):
    lane = lanes()
    row = rows()

    def column(r, carry):
        high, low = carry
        column_ready(r)
        for c in range(N):
            values = [u[a, r, c] for a in range(N)]
            out = along([coeffs[0, a, r, c] for a in range(N)], values)
            for a in range(N):
                total = acc[a, r, c] + out[a]
                acc[a, r, c] = total
                if 0 < c < 6:
                    u_out[a, r, c] = values[a] - scale[a, r, c] * total
        for a in range(N):
            inner = acc[a, r, 0]
            outer = acc[a, r, 6]
            first = inner + jnp.where(lane == 0, 0.0, pltpu.roll(outer, 1, 1))
            last = outer + jnp.where(lane == 127, 0.0, pltpu.roll(inner, 127, 1))
            u_out[a, r, 0] = u[a, r, 0] - scale[a, r, 0] * first
            u_out[a, r, 6] = u[a, r, 6] - scale[a, r, 6] * last
            at = a * N + r
            high = jnp.where(lane == at, pltpu.roll(outer, at + 1, 1), high)
            low = jnp.where(lane == at, pltpu.roll(inner, at, 1), low)
        return high, low

    zero = jnp.zeros((8, 128), jnp.float32)
    high, low = lax.fori_loop(0, N, column, (zero, zero))
    edge_first[...] = jnp.where(where.even, high, low)
    edge_second[...] = jnp.where(where.even, low, high)
    for a in range(N):
        for c in range(N):
            below = jnp.where(row == 0, 0.0, pltpu.roll(acc[a, 6, c], 1, 0))
            above = jnp.where(row == 7, 0.0, pltpu.roll(acc[a, 0, c], 7, 0))
            u_out[a, 0, c] = u_out[a, 0, c] - scale[a, 0, c] * below
            u_out[a, 6, c] = u_out[a, 6, c] - scale[a, 6, c] * above


def send_faces(where, acc, pair, big, small, face):
    side, within, substep = where.side, where.within, where.substep
    upper = upper_of(side)
    lane = lanes()
    for r in range(N):
        for c in range(N):
            pair[r, c] = acc[upper, r, c]

    def from_rotor(table, _):
        def row(r, _):
            values = [acc[6, r, n] for n in range(N)]
            for m in range(N):
                face[r * N + m] = sparse_dot([float(x) for x in table[m]], values)
            return 0

        lax.fori_loop(0, N, row, 0)

    for_each_substep(side == 1, substep, from_rotor)

    @pl.when(side == 2)
    def _():
        for r in range(N):
            for m in range(N):
                face[r * N + m] = acc[0, r, m]

    @pl.when((side == 1) | (side == 2))
    def _():
        lefts = left_count(substep)
        shifts = []
        for m in range(N):
            moved = within + jnp.where(m < lefts, 1, 0)
            shifts.append(jnp.where(side == 1, moved, 128 - moved))
        half = jnp.where((within < 64) == (side == 1), 0, 64)
        for at in range(N * N):
            big[at] = pltpu.roll(face[at], lax.rem(shifts[at % N], 128), 1)
        for g in range((N * N + 1) // 2):
            first = pltpu.roll(face[2 * g], lax.rem(shifts[2 * g % N] + half, 128), 1)
            at = min(2 * g + 1, N * N - 1)
            second = pltpu.roll(face[at], lax.rem(shifts[at % N] + 64 + half, 128), 1)
            small[g] = jnp.where(lane < 64, first, second)


def loads(coeffs, reaction, coeffs_v, reaction_v, sems):
    def plane_copies(a):
        return [
            pltpu.make_async_copy(coeffs.at[2, a], coeffs_v.at[2, a], sems.at[a]),
            pltpu.make_async_copy(coeffs.at[1, a], coeffs_v.at[1, a], sems.at[7 + a]),
            pltpu.make_async_copy(reaction.at[a], reaction_v.at[a], sems.at[14 + a]),
        ]

    def column_copy(r):
        return pltpu.make_async_copy(
            coeffs.at[0, :, r], coeffs_v.at[0, :, r], sems.at[21 + r]
        )

    return plane_copies, column_copy


def first_kernel(
    rotation, field, coeffs, reaction, scale,
    u_out, pair, big, small, edge_first, edge_second, scale_v, branch,
    acc, coeffs_v, reaction_v, u, face, sems,
):
    where = place_at(rotation, 0)
    branch[...] = jnp.full((8, 128), branch_of(where), jnp.int32)
    plane_copies, column_copy = loads(coeffs, reaction, coeffs_v, reaction_v, sems)
    field_copies = [pltpu.make_async_copy(field.at[a], u.at[a], sems.at[30 + a]) for a in range(N)]
    scale_copy = pltpu.make_async_copy(scale, scale_v, sems.at[28])
    for i in range(N):
        a = (i + 1) % N
        field_copies[a].start()
        for copy in plane_copies(a):
            copy.start()
    scale_copy.start()
    for r in range(N):
        column_copy(r).start()

    def plane_ready(i, a):
        pltpu.make_async_copy(field.at[a], u.at[a], sems.at[30 + a]).wait()
        for copy in plane_copies(a):
            copy.wait()

    apply_planes(u, coeffs_v, reaction_v, acc, plane_ready)
    scale_copy.wait()
    finish(
        where, u, coeffs_v, scale_v, acc, u_out, edge_first, edge_second,
        lambda r: column_copy(r).wait(),
    )
    send_faces(where, acc, pair, big, small, face)


def step_kernel(
    rotation, at_step, u_in, scale, coeffs, reaction, pair_in, big_in, small_in,
    first_in, second_in,
    u_out, pair, big, small, edge_first, edge_second, _scale, branch,
    acc, coeffs_v, reaction_v, u, big_v, small_v, sems,
):
    step = at_step[0]
    more = step < STEPS - 1
    was = place_at(rotation, step)
    where = place_at(rotation, jnp.minimum(step + 1, STEPS - 1))
    branch[...] = jnp.full((8, 128), branch_of(where), jnp.int32)
    plane_copies, column_copy = loads(coeffs, reaction, coeffs_v, reaction_v, sems)
    big_copy = pltpu.make_async_copy(big_in, big_v, sems.at[28])
    small_copy = pltpu.make_async_copy(small_in, small_v, sems.at[29])
    edges = (first_in, second_in)

    @pl.when(more)
    def _():
        for i in range(N):
            for copy in plane_copies((i + 1) % N):
                copy.start()
            if i == 2:
                big_copy.start()
                small_copy.start()
        for r in range(N):
            column_copy(r).start()

    def faces():
        big_copy.wait()
        small_copy.wait()
        correct_faces(was, scale, pair_in, big_v, small_v, u)

    copy_and_correct_edges(was, scale, edges, u_in, u)

    @pl.when(more)
    def _():
        def plane_ready(i, a):
            for copy in plane_copies(a):
                copy.wait()

            @pl.when(i == N - 2)
            def _():
                faces()

        apply_planes(u, coeffs_v, reaction_v, acc, plane_ready)
        finish(
            where, u, coeffs_v, scale, acc, u_out, edge_first, edge_second,
            lambda r: column_copy(r).wait(),
        )
        send_faces(where, acc, pair, big, small, big_v)

    @pl.when(step == STEPS - 1)
    def _():
        big_copy.start()
        small_copy.start()
        faces()

        def copy(a, _):
            for r in range(N):
                for c in range(N):
                    u_out[a, r, c] = u[a, r, c]
            return 0

        lax.fori_loop(0, N, copy, 0)


def at(circ, side):
    return (circ % CIRC) * SIDES + side


EVERY = [(c, s) for c in range(CIRC) for s in range(SIDES)]
PAIR = [(at(c, s), at(c, s ^ 1)) for c, s in EVERY]
SWAP_FIRST = [(at(c, s), at(c ^ 1, s)) for c, s in EVERY]
SWAP_SECOND = [(at(c, s), at(c + (1 if c % 2 else -1), s)) for c, s in EVERY]


def rotated(hops):
    pairs = []
    for c in range(CIRC):
        pairs.append((at(c, 1), at(c + hops, 2)))
        pairs.append((at(c, 2), at(c - hops, 1)))
    return pairs


def exchange(big_hops, small_hops, big, small):
    big = lax.ppermute(big, AXES, rotated(big_hops))
    return big, lax.ppermute(small, AXES, rotated(small_hops))


def local(field, coeffs, reaction, step_scale, rotation):
    field, coeffs, reaction, step_scale = field[0], coeffs[0], reaction[0], step_scale[0]
    branches = [lambda *v, h=h: exchange(h, h + 1, *v) for h in range(CIRC)]
    branches += [lambda *v, h=h: exchange(h + 1, h, *v) for h in range(CIRC)]

    array = lambda *shape: jax.ShapeDtypeStruct(shape, jnp.float32)
    node = pltpu.VMEM(field.shape, jnp.float32)
    face, edge = array(*field.shape[1:]), array(8, 128)
    sends = (node, face, array(49, 8, 128), array(25, 8, 128), edge, edge, node)
    sends += (jax.ShapeDtypeStruct((8, 128), jnp.int32),)
    vmem = pl.BlockSpec(memory_space=pltpu.VMEM)
    smem = pl.BlockSpec(memory_space=pltpu.SMEM)
    hbm = pl.BlockSpec(memory_space=pltpu.HBM)
    buffers = [pltpu.VMEM(shape, jnp.float32) for shape in (field.shape, coeffs.shape, field.shape)]
    bigger = pltpu.VMEM((49, 8, 128), jnp.float32)
    params = pltpu.CompilerParams(vmem_limit_bytes=VMEM_LIMIT)
    field, coeffs, reaction, step_scale = [
        pltpu.with_memory_space_constraint(x, pltpu.HBM)
        for x in (field, coeffs, reaction, step_scale)
    ]
    carry = pl.pallas_call(
        first_kernel,
        out_shape=sends,
        in_specs=[smem] + [hbm] * 4,
        out_specs=(vmem,) * 8,
        scratch_shapes=buffers + [buffers[0], bigger, pltpu.SemaphoreType.DMA((37,))],
        compiler_params=params,
        name="first",
    )(rotation, field, coeffs, reaction, step_scale)
    advance = pl.pallas_call(
        step_kernel,
        out_shape=sends,
        in_specs=[smem, smem, vmem, vmem, hbm, hbm, vmem, hbm, hbm, vmem, vmem],
        out_specs=(vmem,) * 8,
        scratch_shapes=buffers
        + [buffers[0], bigger, pltpu.VMEM((25, 8, 128), jnp.float32)]
        + [pltpu.SemaphoreType.DMA((30,))],
        input_output_aliases={2: 0, 3: 6},
        compiler_params=params,
        name="step",
    )

    def body(step, carry):
        u, pair, big, small, first, second, scale, branch = carry
        pair = lax.ppermute(pair, AXES, PAIR)
        first = lax.ppermute(first, AXES, SWAP_FIRST)
        second = lax.ppermute(second, AXES, SWAP_SECOND)
        big, small = lax.switch(branch[0, 0], branches, big, small)
        streamed = [pltpu.with_memory_space_constraint(x, pltpu.HBM) for x in (coeffs, reaction)]
        return advance(
            rotation, step[None], u, scale, *streamed, pair, big, small, first, second
        )

    return lax.fori_loop(0, STEPS, body, tuple(carry))[0][None]


def solution(mesh):
    in_specs = (
        P("side", None, None, None, None, "circ"),
        P("side", None, None, None, None, None, "circ"),
        P("side", None, None, None, None, "circ"),
        P("side", None, None, None, None, "circ"),
        P(),
    )
    out_specs = P("side", None, None, None, None, "circ")
    return jax.shard_map(local, mesh=mesh, in_specs=in_specs, out_specs=out_specs, check_vma=False)
```

```python
from typing import NamedTuple

import jax
import jax.numpy as jnp
import numpy as np
from jax import lax
from jax.experimental import pallas as pl
from jax.experimental.pallas import tpu as pltpu
from jax.sharding import PartitionSpec as P

SUBSTEPS = 3
STEPS = 4
N = 7
CIRC = 32
SIDES = 4
VMEM_LIMIT = 16 * 2**20
AXES = ("circ", "side")


def gll_points():
    return np.array(
        [
            -1.0,
            -0.830223896278567,
            -0.4688487934707142,
            0.0,
            0.4688487934707142,
            0.830223896278567,
            1.0,
        ]
    )


def derivative_table():
    points = gll_points()
    weights = np.array(
        [1.0 / np.prod([points[j] - points[k] for k in range(N) if k != j]) for j in range(N)]
    )
    derivative = np.zeros((N, N))
    for i in range(N):
        for j in range(N):
            if i != j:
                derivative[i, j] = weights[j] / weights[i] / (points[i] - points[j])
        derivative[i, i] = -np.sum(derivative[i])
    return derivative


def mortar_table(substep):
    points = gll_points()
    heights = (1.0 + points) * 0.5
    fraction = substep / SUBSTEPS
    on_right = heights >= fraction
    local = 2.0 * np.where(on_right, heights - fraction, heights - fraction + 1.0) - 1.0
    table = np.array(
        [
            [
                np.prod([(at - points[q]) / (points[n] - points[q]) for q in range(N) if q != n])
                for n in range(N)
            ]
            for at in local
        ]
    )
    return table, ~on_right


D = derivative_table()
EVEN = [[float(0.5 * (D[p, q] + D[p, 6 - q])) for q in range(3)] for p in range(3)]
ODD = [[float(0.5 * (D[p, q] - D[p, 6 - q])) for q in range(3)] for p in range(3)]
TO_MID = [float(D[3, q]) for q in range(3)]
FROM_MID = [float(D[p, 3]) for p in range(3)]
TABLES = [mortar_table(substep) for substep in range(SUBSTEPS)]


def dot(weights, values):
    total = weights[0] * values[0]
    for weight, value in zip(weights[1:], values[1:]):
        total = total + weight * value
    return total


def differentiate(v):
    s = [v[i] + v[6 - i] for i in range(3)]
    d = [v[i] - v[6 - i] for i in range(3)]
    odd = [dot(EVEN[p] + [FROM_MID[p]], s + [v[3]]) for p in range(3)]
    even = [dot(ODD[p], d) for p in range(3)]
    mid = dot(TO_MID, d)
    return (
        [even[p] + odd[p] for p in range(3)] + [mid] + [even[p] - odd[p] for p in (2, 1, 0)]
    )


def differentiate_transposed(w):
    s = [w[i] + w[6 - i] for i in range(3)]
    d = [w[i] - w[6 - i] for i in range(3)]
    odd = [dot([ODD[p][q] for p in range(3)] + [TO_MID[q]], s + [w[3]]) for q in range(3)]
    even = [dot([EVEN[p][q] for p in range(3)], d) for q in range(3)]
    mid = dot(FROM_MID, d)
    return (
        [even[q] + odd[q] for q in range(3)] + [mid] + [even[q] - odd[q] for q in (2, 1, 0)]
    )


def along(coeffs, values):
    grad = differentiate(values)
    return differentiate_transposed([c * g for c, g in zip(coeffs, grad)])


def sparse_dot(weights, values):
    terms = [v if w == 1.0 else w * v for w, v in zip(weights, values) if w != 0.0]
    total = terms[0]
    for term in terms[1:]:
        total = total + term
    return total


def lanes():
    return lax.broadcasted_iota(jnp.int32, (8, 128), 1)


def rows():
    return lax.broadcasted_iota(jnp.int32, (8, 128), 0)


class Place(NamedTuple):
    side: jax.Array
    even: jax.Array
    sector: jax.Array
    within: jax.Array
    substep: jax.Array


def place_at(rotation, step):
    whole = lax.div(rotation[step], SUBSTEPS)
    return Place(
        side=lax.axis_index("side"),
        even=lax.rem(lax.axis_index("circ"), 2) == 0,
        sector=lax.div(whole, 128),
        within=lax.rem(whole, 128),
        substep=rotation[step] - SUBSTEPS * whole,
    )


def branch_of(place):
    return place.sector + jnp.where(place.within < 64, 0, CIRC)


def upper_of(side):
    return jnp.where(side % 2 == 0, 6, 0)


def for_each_substep(condition, substep, run):
    for value in range(SUBSTEPS):

        @pl.when(condition & (substep == value))
        def _(value=value):
            table, left = TABLES[value]
            run(table, [int(is_left) for is_left in left])


def copy_and_correct_edges(place, scale, edges, u_in, u):
    lane = lanes()
    first, second = [edge[...] for edge in edges]
    high = jnp.where(place.even, second, first)
    low = jnp.where(place.even, first, second)
    for a in range(N):
        for r in range(N):
            at = a * N + r
            from_low = jnp.where(lane == 0, pltpu.roll(low, (128 - at) % 128, 1), 0.0)
            from_high = jnp.where(lane == 127, pltpu.roll(high, 127 - at, 1), 0.0)
            for c in range(1, 6):
                u[a, r, c] = u_in[a, r, c]
            u[a, r, 0] = u_in[a, r, 0] - scale[a, r, 0] * from_low
            u[a, r, 6] = u_in[a, r, 6] - scale[a, r, 6] * from_high


def left_count(substep):
    counts = [int(left.sum()) for _, left in TABLES]
    return jnp.where(substep == 0, counts[0], jnp.where(substep == 1, counts[1], counts[2]))


def correct_faces(where, scale, pair, big, small, u):
    side, within, substep = where.side, where.within, where.substep
    upper = upper_of(side)
    lane = lanes()
    for r in range(N):
        for c in range(N):
            u[upper, r, c] = u[upper, r, c] - scale[upper, r, c] * pair[r, c]

    @pl.when((side == 1) | (side == 2))
    def _():
        low = (within < 64) == (side == 2)
        place = jnp.where(low, lane, 127 - lane)
        turns = [jnp.where(low, 0, 64), jnp.where(low, 64, 0)]
        lefts = left_count(substep)
        limits = []
        for m in range(N):
            moved = within + jnp.where(m < lefts, 1, 0)
            first = jnp.where(side == 2, moved, 128 - moved)
            limits.append(jnp.where(low, first, 128 - first))
        for at in range(N * N):
            half = pltpu.roll(small[at // 2], turns[at % 2], 1)
            big[at] = jnp.where(place < limits[at % N], half, big[at])

    @pl.when(side == 2)
    def _():
        for r in range(N):
            for m in range(N):
                u[0, r, m] = u[0, r, m] - scale[0, r, m] * big[r * N + m]

    def to_rotor(table, _):
        def add(r, _):
            parts = [big[r * N + m] for m in range(N)]
            for n in range(N):
                part = sparse_dot([float(table[m, n]) for m in range(N)], parts)
                u[6, r, n] = u[6, r, n] - scale[6, r, n] * part
            return 0

        lax.fori_loop(0, N, add, 0)

    for_each_substep(side == 1, substep, to_rotor)


def apply_planes(u, coeffs, reaction, acc, plane_ready):
    def plane(i, _):
        a = lax.rem(i + 1, N)
        plane_ready(i, a)
        for r in range(N):
            values = [u[a, r, c] for c in range(N)]
            out = along([coeffs[2, a, r, c] for c in range(N)], values)
            for c in range(N):
                acc[a, r, c] = out[c] + reaction[a, r, c] * values[c]
        for c in range(N):
            out = along(
                [coeffs[1, a, r, c] for r in range(N)], [u[a, r, c] for r in range(N)]
            )
            for r in range(N):
                acc[a, r, c] = acc[a, r, c] + out[r]
        return 0

    lax.fori_loop(0, N, plane, 0)


def finish(where, u, coeffs, scale, acc, u_out, edge_first, edge_second, column_ready):
    lane = lanes()
    row = rows()

    def column(r, carry):
        high, low = carry
        column_ready(r)
        for c in range(N):
            values = [u[a, r, c] for a in range(N)]
            out = along([coeffs[0, a, r, c] for a in range(N)], values)
            for a in range(N):
                total = acc[a, r, c] + out[a]
                acc[a, r, c] = total
                if 0 < c < 6:
                    u_out[a, r, c] = values[a] - scale[a, r, c] * total
        for a in range(N):
            inner = acc[a, r, 0]
            outer = acc[a, r, 6]
            first = inner + jnp.where(lane == 0, 0.0, pltpu.roll(outer, 1, 1))
            last = outer + jnp.where(lane == 127, 0.0, pltpu.roll(inner, 127, 1))
            u_out[a, r, 0] = u[a, r, 0] - scale[a, r, 0] * first
            u_out[a, r, 6] = u[a, r, 6] - scale[a, r, 6] * last
            at = a * N + r
            high = jnp.where(lane == at, pltpu.roll(outer, at + 1, 1), high)
            low = jnp.where(lane == at, pltpu.roll(inner, at, 1), low)
        return high, low

    zero = jnp.zeros((8, 128), jnp.float32)
    high, low = lax.fori_loop(0, N, column, (zero, zero))
    edge_first[...] = jnp.where(where.even, low, high)
    edge_second[...] = jnp.where(where.even, high, low)
    for a in range(N):
        for c in range(N):
            below = jnp.where(row == 0, 0.0, pltpu.roll(acc[a, 6, c], 1, 0))
            above = jnp.where(row == 7, 0.0, pltpu.roll(acc[a, 0, c], 7, 0))
            u_out[a, 0, c] = u_out[a, 0, c] - scale[a, 0, c] * below
            u_out[a, 6, c] = u_out[a, 6, c] - scale[a, 6, c] * above


def send_faces(where, acc, pair, big, small, face):
    side, within, substep = where.side, where.within, where.substep
    upper = upper_of(side)
    lane = lanes()
    for r in range(N):
        for c in range(N):
            pair[r, c] = acc[upper, r, c]

    def from_rotor(table, _):
        def row(r, _):
            values = [acc[6, r, n] for n in range(N)]
            for m in range(N):
                face[r * N + m] = sparse_dot([float(x) for x in table[m]], values)
            return 0

        lax.fori_loop(0, N, row, 0)

    for_each_substep(side == 1, substep, from_rotor)

    @pl.when(side == 2)
    def _():
        for r in range(N):
            for m in range(N):
                face[r * N + m] = acc[0, r, m]

    @pl.when((side == 1) | (side == 2))
    def _():
        lefts = left_count(substep)
        shifts = []
        for m in range(N):
            moved = within + jnp.where(m < lefts, 1, 0)
            shifts.append(jnp.where(side == 1, moved, 128 - moved))
        half = jnp.where((within < 64) == (side == 1), 0, 64)
        for at in range(N * N):
            big[at] = pltpu.roll(face[at], lax.rem(shifts[at % N], 128), 1)
        for g in range((N * N + 1) // 2):
            first = pltpu.roll(face[2 * g], lax.rem(shifts[2 * g % N] + half, 128), 1)
            at = min(2 * g + 1, N * N - 1)
            second = pltpu.roll(face[at], lax.rem(shifts[at % N] + 64 + half, 128), 1)
            small[g] = jnp.where(lane < 64, first, second)


def loads(coeffs, reaction, coeffs_v, reaction_v, sems):
    def plane_copies(a):
        return [
            pltpu.make_async_copy(coeffs.at[2, a], coeffs_v.at[2, a], sems.at[a]),
            pltpu.make_async_copy(coeffs.at[1, a], coeffs_v.at[1, a], sems.at[7 + a]),
            pltpu.make_async_copy(reaction.at[a], reaction_v.at[a], sems.at[14 + a]),
        ]

    def column_copy(r):
        return pltpu.make_async_copy(
            coeffs.at[0, :, r], coeffs_v.at[0, :, r], sems.at[21 + r]
        )

    return plane_copies, column_copy


def first_kernel(
    rotation, field, coeffs, reaction, scale,
    u_out, pair, big, small, edge_first, edge_second, scale_v, branch,
    acc, coeffs_v, reaction_v, u, face, sems,
):
    where = place_at(rotation, 0)
    branch[...] = jnp.full((8, 128), branch_of(where), jnp.int32)
    plane_copies, column_copy = loads(coeffs, reaction, coeffs_v, reaction_v, sems)
    field_copies = [pltpu.make_async_copy(field.at[a], u.at[a], sems.at[30 + a]) for a in range(N)]
    scale_copy = pltpu.make_async_copy(scale, scale_v, sems.at[28])
    for i in range(N):
        a = (i + 1) % N
        field_copies[a].start()
        for copy in plane_copies(a):
            copy.start()
    scale_copy.start()
    for r in range(N):
        column_copy(r).start()

    def plane_ready(i, a):
        pltpu.make_async_copy(field.at[a], u.at[a], sems.at[30 + a]).wait()
        for copy in plane_copies(a):
            copy.wait()

    apply_planes(u, coeffs_v, reaction_v, acc, plane_ready)
    scale_copy.wait()
    finish(
        where, u, coeffs_v, scale_v, acc, u_out, edge_first, edge_second,
        lambda r: column_copy(r).wait(),
    )
    send_faces(where, acc, pair, big, small, face)


def step_kernel(
    rotation, at_step, u_in, scale, coeffs, reaction, pair_in, big_in, small_in,
    first_in, second_in,
    u_out, pair, big, small, edge_first, edge_second, _scale, branch,
    acc, coeffs_v, reaction_v, u, big_v, small_v, sems,
):
    step = at_step[0]
    more = step < STEPS - 1
    was = place_at(rotation, step)
    where = place_at(rotation, jnp.minimum(step + 1, STEPS - 1))
    branch[...] = jnp.full((8, 128), branch_of(where), jnp.int32)
    plane_copies, column_copy = loads(coeffs, reaction, coeffs_v, reaction_v, sems)
    big_copy = pltpu.make_async_copy(big_in, big_v, sems.at[28])
    small_copy = pltpu.make_async_copy(small_in, small_v, sems.at[29])
    edges = (first_in, second_in)

    @pl.when(more)
    def _():
        for i in range(N):
            for copy in plane_copies((i + 1) % N):
                copy.start()
            if i == 2:
                big_copy.start()
                small_copy.start()
        for r in range(N):
            column_copy(r).start()

    def faces():
        big_copy.wait()
        small_copy.wait()
        correct_faces(was, scale, pair_in, big_v, small_v, u)

    copy_and_correct_edges(was, scale, edges, u_in, u)

    @pl.when(more)
    def _():
        def plane_ready(i, a):
            for copy in plane_copies(a):
                copy.wait()

            @pl.when(i == N - 2)
            def _():
                faces()

        apply_planes(u, coeffs_v, reaction_v, acc, plane_ready)
        finish(
            where, u, coeffs_v, scale, acc, u_out, edge_first, edge_second,
            lambda r: column_copy(r).wait(),
        )
        send_faces(where, acc, pair, big, small, big_v)

    @pl.when(step == STEPS - 1)
    def _():
        big_copy.start()
        small_copy.start()
        faces()

        def copy(a, _):
            for r in range(N):
                for c in range(N):
                    u_out[a, r, c] = u[a, r, c]
            return 0

        lax.fori_loop(0, N, copy, 0)


def at(circ, side):
    return (circ % CIRC) * SIDES + side


EVERY = [(c, s) for c in range(CIRC) for s in range(SIDES)]
PAIR = [(at(c, s), at(c, s ^ 1)) for c, s in EVERY]
SWAP_FIRST = [(at(c, s), at(c ^ 1, s)) for c, s in EVERY]
SWAP_SECOND = [(at(c, s), at(c + (1 if c % 2 else -1), s)) for c, s in EVERY]


def rotated(hops):
    pairs = []
    for c in range(CIRC):
        pairs.append((at(c, 1), at(c + hops, 2)))
        pairs.append((at(c, 2), at(c - hops, 1)))
    return pairs


def exchange(big_hops, small_hops, big, small):
    big = lax.ppermute(big, AXES, rotated(big_hops))
    return big, lax.ppermute(small, AXES, rotated(small_hops))


def local(field, coeffs, reaction, step_scale, rotation):
    field, coeffs, reaction, step_scale = field[0], coeffs[0], reaction[0], step_scale[0]
    branches = [lambda *v, h=h: exchange(h, h + 1, *v) for h in range(CIRC)]
    branches += [lambda *v, h=h: exchange(h + 1, h, *v) for h in range(CIRC)]

    array = lambda *shape: jax.ShapeDtypeStruct(shape, jnp.float32)
    node = pltpu.VMEM(field.shape, jnp.float32)
    face, edge = array(*field.shape[1:]), array(8, 128)
    sends = (node, face, array(49, 8, 128), array(25, 8, 128), edge, edge, node)
    sends += (jax.ShapeDtypeStruct((8, 128), jnp.int32),)
    vmem = pl.BlockSpec(memory_space=pltpu.VMEM)
    smem = pl.BlockSpec(memory_space=pltpu.SMEM)
    hbm = pl.BlockSpec(memory_space=pltpu.HBM)
    buffers = [pltpu.VMEM(shape, jnp.float32) for shape in (field.shape, coeffs.shape, field.shape)]
    bigger = pltpu.VMEM((49, 8, 128), jnp.float32)
    params = pltpu.CompilerParams(vmem_limit_bytes=VMEM_LIMIT)
    field, coeffs, reaction, step_scale = [
        pltpu.with_memory_space_constraint(x, pltpu.HBM)
        for x in (field, coeffs, reaction, step_scale)
    ]
    carry = pl.pallas_call(
        first_kernel,
        out_shape=sends,
        in_specs=[smem] + [hbm] * 4,
        out_specs=(vmem,) * 8,
        scratch_shapes=buffers + [buffers[0], bigger, pltpu.SemaphoreType.DMA((37,))],
        compiler_params=params,
        name="first",
    )(rotation, field, coeffs, reaction, step_scale)
    advance = pl.pallas_call(
        step_kernel,
        out_shape=sends,
        in_specs=[smem, smem, vmem, vmem, hbm, hbm, vmem, hbm, hbm, vmem, vmem],
        out_specs=(vmem,) * 8,
        scratch_shapes=buffers
        + [buffers[0], bigger, pltpu.VMEM((25, 8, 128), jnp.float32)]
        + [pltpu.SemaphoreType.DMA((30,))],
        input_output_aliases={2: 0, 3: 6},
        compiler_params=params,
        name="step",
    )

    def body(step, carry):
        u, pair, big, small, first, second, scale, branch = carry
        pair = lax.ppermute(pair, AXES, PAIR)
        first = lax.ppermute(first, AXES, SWAP_SECOND)
        second = lax.ppermute(second, AXES, SWAP_FIRST)
        big, small = lax.switch(branch[0, 0], branches, big, small)
        streamed = [pltpu.with_memory_space_constraint(x, pltpu.HBM) for x in (coeffs, reaction)]
        return advance(
            rotation, step[None], u, scale, *streamed, pair, big, small, first, second
        )

    return lax.fori_loop(0, STEPS, body, tuple(carry))[0][None]


def solution(mesh):
    in_specs = (
        P("side", None, None, None, None, "circ"),
        P("side", None, None, None, None, None, "circ"),
        P("side", None, None, None, None, "circ"),
        P("side", None, None, None, None, "circ"),
        P(),
    )
    out_specs = P("side", None, None, None, None, "circ")
    return jax.shard_map(local, mesh=mesh, in_specs=in_specs, out_specs=out_specs, check_vma=False)
```
